32 devices in a mesh: dp: 8 (over y, x, core), tensor: 4 (over z).
Axes of the slice: x: 2, y: 2, z: 4, core: 2. Of those that a mesh axis runs over, the one named last changes fastest.
Arguments:
- tokens: bfloat16 [128, 5376], P('dp'), may hold values from -6 to 6
- lengths: int32 [128], P('dp'), may hold values from 1 to 1024, as said below
- positions: int32 [128], P('dp'), may hold values from 1 to 33791, as said below
- in_gain: float32 [5376], replicated, may hold values from 0.25 to 1.75
- q_weight: bfloat16 [5376, 4096], P('dp', 'tensor'), may hold values from -0.078125 to 0.078125
- k_weight: bfloat16 [5376, 2048], P('dp', 'tensor'), may hold values from -0.078125 to 0.078125
- v_weight: bfloat16 [5376, 2048], P('dp', 'tensor'), may hold values from -0.078125 to 0.078125
- q_gain: float32 [128], replicated, may hold values from 0.1 to 1.9
- k_gain: float32 [128], replicated, may hold values from 0.1 to 1.9
- key_cache: bfloat16 [128, 1024, 2048], P('dp', None, 'tensor'), may hold values from -480 to 480
- value_cache: bfloat16 [128, 1024, 2048], P('dp', None, 'tensor'), may hold values from -6 to 6
- out_weight: bfloat16 [4096, 5376], P('tensor', 'dp'), may hold values from -0.09375 to 0.09375
- post_gain: float32 [5376], replicated, may hold values from 0.25 to 1.75
Outputs:
- hidden_out: bfloat16 [128, 5376], P('dp')
- new_keys: bfloat16 [128, 2048], P('dp', 'tensor')
- new_values: bfloat16 [128, 2048], P('dp', 'tensor')
The draws below stay inside these ranges and needn't reach their ends.
Inputs may be any that keep to these rules, and one draw needn't show every extreme that they name: Slots 0 to lengths - 1 of a sequence hold its cache; some sequence has exactly 1024. `positions`: each position is at least the sequence's length.
All inputs are finite; a program needn't handle non-finite values.
Results may differ from the reference program's by a relative error of at most 0.012.
The reference program's roundings to bfloat16 on the way count: a program that leaves them out, or rounds other values in their place, can miss the bound.
Values may be sent and summed in bfloat16 or wider, within the bound.
A program may use at most 64 MiB of HBM per device.

```python
import jax
import jax.numpy as jnp
from jax import lax

D = 5376
H = 32
KV = 16
HD = 128
QPRE = 168
BSEQ = 16
CTX = 1024
BATCH = 128


def length_table(key):
    groups = BATCH // BSEQ
    key_one, key_two, key_three, key_four = jax.random.split(jax.random.fold_in(key, 7), 4)
    ceiling = jax.random.randint(key_one, (groups, 1), max(CTX // 8, 1), CTX + 1)
    raw_draws = jax.random.randint(key_two, (groups, BSEQ), 0, 1 << 30)
    filled = (1 + raw_draws % ceiling).reshape(BATCH)
    chosen = jax.random.randint(key_three, (), 0, BATCH)
    filled = jnp.where(jnp.arange(BATCH) == chosen, CTX, filled)
    shifts = jax.random.randint(key_four, (BATCH,), 0, 32768)
    return (filled.astype(jnp.int32), (filled + shifts).astype(jnp.int32))


def draw_lengths(key, part):
    return length_table(key)[0]


def draw_positions(key, part):
    return length_table(key)[1]


def draw_key_cache(key, part):
    key_one, key_two = jax.random.split(jax.random.fold_in(key, 13))
    normal = 3.0 * jax.random.truncated_normal(key_one, -4.0, 4.0, (BATCH, CTX, KV * HD), jnp.float32)
    return normal.astype(jnp.bfloat16)


def steps_of(stream_key, shape, cuts, least, top_value):
    level = 1.0
    for axis_at, blocks in cuts:
        heights = jax.random.uniform(jax.random.fold_in(jax.random.fold_in(stream_key, 6), axis_at), (blocks,), jnp.float32, least / len(cuts), top_value / len(cuts))
        level = level * jnp.repeat(jnp.exp(heights), shape[axis_at] // blocks).reshape((-1,) + (1,) * (len(shape) - 1 - axis_at))
    return level


def noise(key, extent, width, limit, shards=(), held_as=jnp.bfloat16):
    entries = width * jax.random.normal(key, extent, jnp.float32)
    if shards:
        entries = entries * steps_of(key, extent, shards, -0.22, 0.18)
    return jnp.clip(entries, -limit, limit).astype(held_as)


def setup_inputs(seed: int = 0) -> dict:
    arg_keys = jax.random.split(jax.random.key(seed), 14)
    tokens = noise(arg_keys[0], (BATCH, D), 1.0, 6.0, ((0, 8),))
    lengths = draw_lengths(jax.random.fold_in(arg_keys[13], 71), 0)
    positions = draw_positions(jax.random.fold_in(arg_keys[13], 71), 0)
    in_gain = jnp.clip(1.0 + 0.15 * jax.random.normal(arg_keys[3], (D,), jnp.float32), 0.25, 1.75)
    q_weight = noise(arg_keys[4], (D, H * HD), D ** -0.5, 0.078125, ((0, 8), (1, 4)))
    k_weight = noise(arg_keys[5], (D, KV * HD), D ** -0.5, 0.078125, ((0, 8), (1, 4)))
    v_weight = noise(arg_keys[6], (D, KV * HD), D ** -0.5, 0.078125, ((0, 8), (1, 4)))
    q_gain = jnp.clip(1.0 + 0.18 * jax.random.normal(arg_keys[7], (HD,), jnp.float32), 0.1, 1.9)
    k_gain = jnp.clip(1.0 + 0.18 * jax.random.normal(arg_keys[8], (HD,), jnp.float32), 0.1, 1.9)
    key_cache = draw_key_cache(jax.random.fold_in(arg_keys[13], 71), 0)
    value_cache = noise(arg_keys[10], (BATCH, CTX, KV * HD), 1.0, 6.0, ((0, 8), (2, 4)))
    out_weight = noise(arg_keys[11], (H * HD, D), (H * HD) ** -0.5, 0.09375, ((0, 4), (1, 8)))
    post_gain = jnp.clip(1.0 + 0.15 * jax.random.normal(arg_keys[12], (D,), jnp.float32), 0.25, 1.75)
    return dict(tokens=tokens, lengths=lengths, positions=positions, in_gain=in_gain, q_weight=q_weight, k_weight=k_weight, v_weight=v_weight, q_gain=q_gain, k_gain=k_gain, key_cache=key_cache, value_cache=value_cache, out_weight=out_weight, post_gain=post_gain)


epsilon = 1e-06
rope_base = 1000000.0
rope_factor = 8.0

def rms_scale(vectors, gain):
    mean_square = lax.optimization_barrier(jnp.mean(vectors * vectors, axis=-1, keepdims=True))
    return vectors * lax.rsqrt(mean_square + epsilon) * gain

def rotate(vectors, positions):
    half_width = vectors.shape[-1] // 2
    exponent = jnp.arange(half_width, dtype=jnp.float32) * (2.0 / vectors.shape[-1])
    frequency = jnp.power(rope_base, -exponent)
    angles = (positions.astype(jnp.float32) / rope_factor)[:, None] * frequency[None, :]
    cos_part = jnp.cos(angles)[:, None, :]
    sin_part = jnp.sin(angles)[:, None, :]
    first_half = vectors[..., :half_width]
    second_half = vectors[..., half_width:]
    return jnp.concatenate([first_half * cos_part - second_half * sin_part, second_half * cos_part + first_half * sin_part], axis=-1)

def reference(tokens, lengths, positions, in_gain, q_weight, k_weight, v_weight, q_gain, k_gain, key_cache, value_cache, out_weight, post_gain):
    batch_size = tokens.shape[0]
    per_group = H // KV
    normed = rms_scale(tokens.astype(jnp.float32), in_gain).astype(jnp.bfloat16)
    q_raw = jnp.dot(normed, q_weight, preferred_element_type=jnp.float32).reshape(batch_size, H, HD)
    k_raw = jnp.dot(normed, k_weight, preferred_element_type=jnp.float32).reshape(batch_size, KV, HD)
    v_raw = jnp.dot(normed, v_weight, preferred_element_type=jnp.float32)
    new_values = v_raw.astype(jnp.bfloat16)
    queries = (rotate(rms_scale(q_raw, q_gain), positions) * QPRE ** (-0.5)).astype(jnp.bfloat16)
    new_keys = rotate(rms_scale(k_raw, k_gain), positions).astype(jnp.bfloat16).reshape(batch_size, KV * HD)

    def attend(sequence):
        query_row, key_own, value_own, cache_keys, cache_values, length = sequence
        grouped = query_row.astype(jnp.float32).reshape(KV, per_group, HD)
        keys_f = cache_keys.astype(jnp.float32).reshape(CTX, KV, HD)
        values_f = cache_values.astype(jnp.float32).reshape(CTX, KV, HD)
        scores = jnp.einsum('grd,jgd->grj', grouped, keys_f)
        usable = jnp.arange(CTX) < length
        scores = jnp.where(usable[None, None, :], scores, -jnp.inf)
        self_score = jnp.einsum('grd,gd->gr', grouped, key_own.astype(jnp.float32).reshape(KV, HD))
        largest = jnp.maximum(lax.optimization_barrier(jnp.max(scores, axis=-1)), self_score)
        weights = jnp.exp(scores - largest[..., None])
        self_weight = jnp.exp(self_score - largest)
        running = lax.optimization_barrier(jnp.sum(weights, axis=-1)) + self_weight
        rounded = lax.optimization_barrier(weights.astype(jnp.bfloat16)).astype(jnp.float32)
        rounded_self = lax.optimization_barrier(self_weight.astype(jnp.bfloat16)).astype(jnp.float32)
        mixture = jnp.einsum('grj,jgd->grd', rounded, values_f)
        mixture = mixture + rounded_self[..., None] * value_own.astype(jnp.float32).reshape(KV, 1, HD)
        return (mixture / running[..., None]).reshape(H * HD).astype(jnp.bfloat16)
    attended = lax.map(attend, (queries, new_keys, new_values, key_cache, value_cache, lengths))
    projected = jnp.dot(attended, out_weight, preferred_element_type=jnp.float32)
    hidden_out = (tokens.astype(jnp.float32) + rms_scale(projected, post_gain)).astype(jnp.bfloat16)
    return (hidden_out, new_keys, new_values)
```

```python
import functools

import jax
import jax.numpy as jnp
import numpy as np
from jax import lax
from jax.experimental import pallas as pl
from jax.experimental.pallas import tpu as pltpu
from jax.sharding import PartitionSpec as P

HD = 128
QPRE = 168
LIMIT = 54000000
CHUNKS = 4
EARLY = 4
READY = 12

epsilon = 1e-06
rope_base = 1000000.0
rope_factor = 8.0

MESH = pl.DeviceIdType.MESH
VMEM = pltpu.VMEM
SMEM = pltpu.SMEM
F32 = jnp.float32
BF16 = jnp.bfloat16


def flip(a, b, n):
    total, bit = 0, 1
    while bit < n:
        total = total + lax.rem(a // bit + b // bit, 2) * bit
        bit *= 2
    return total


def layer_kernel(
    n, m, tok_hbm, len_hbm, pos_hbm, freq_hbm, gain_hbm, wq_hbm, wk_hbm, wv_hbm, qg_hbm, kg_hbm,
    kc_hbm, vc_hbm, wo_hbm, post_hbm,
    hid_out, nk_out, nv_out,
    tok_v, len_s, pos_s, tables, gains, w, kbuf, vbuf, turned, wo, wt,
    sbuf, rbuf, keep, pout, pin, rs, rr, q_s, kx_s, vx_s, scores, weights, sums, owns, mixed,
    att, gath, ps, pr, fs, fr,
    lsem, wsem, ksem, vsem, osem, s1, r1, sp, rp, s2, r2, s3, r3, s4, r4, s5, r5,
):
    me = lax.axis_index("dp")
    mt = lax.axis_index("tensor")
    rows, width = tok_v.shape
    depth, cols = w.shape
    qc, kc = wq_hbm.shape[1], wk_hbm.shape[1]
    ctx = kbuf.shape[1]
    ocols = wo.shape[0]
    heads, groups = qc // HD, kc // HD
    per = heads // groups
    half = n // 2
    part = rows // CHUNKS
    ready = turned.shape[0]
    chunk = min(512, cols)
    chunks = cols // chunk

    barrier = pltpu.get_barrier_semaphore()
    for a in range(1, n):
        pl.semaphore_signal(
            barrier, inc=1, device_id={"dp": lax.rem(me + a, n), "tensor": mt}, device_id_type=MESH)
    for b in range(1, m):
        pl.semaphore_signal(
            barrier, inc=1, device_id={"dp": me, "tensor": lax.rem(mt + b, m)}, device_id_type=MESH)

    copy = pltpu.make_async_copy
    small = [
        copy(tok_hbm, tok_v, lsem.at[0]),
        copy(gain_hbm, gains.at[0], lsem.at[1]),
        copy(post_hbm, gains.at[1], lsem.at[1]),
        copy(qg_hbm, tables.at[0], lsem.at[2]),
        copy(kg_hbm, tables.at[1], lsem.at[2]),
        copy(freq_hbm, tables.at[2], lsem.at[2]),
        copy(len_hbm, len_s, lsem.at[3]),
        copy(pos_hbm, pos_s, lsem.at[4]),
    ]
    loads = [
        copy(wq_hbm, w.at[:, pl.ds(0, qc)], wsem.at[0]),
        copy(wk_hbm, w.at[:, pl.ds(qc, kc)], wsem.at[1]),
        copy(wv_hbm, w.at[:, pl.ds(qc + kc, kc)], wsem.at[1]),
    ]
    keys = [copy(kc_hbm.at[b], kbuf.at[b % ready], ksem.at[b // 2]) for b in range(rows)]
    values = [copy(vc_hbm.at[b], vbuf.at[b], vsem.at[b // 2]) for b in range(rows)]

    def settle(ref, sem):
        copy(ref, ref, sem).wait()

    wload = copy(wo_hbm, wo, osem)
    for load in small + loads + [wload]:
        load.start()

    with jax.named_scope("norm"):
        with jax.named_scope("tokwait"):
            settle(tok_v, lsem.at[0])
        settle(gains, lsem.at[1])
        for load in keys[:EARLY]:
            load.start()
        tok = tok_v[...].astype(F32)
        scale = lax.rsqrt(jnp.sum(tok * tok, axis=-1, keepdims=True) * (1.0 / width) + epsilon)
        normed = jnp.concatenate([
            (tok[:, k * HD : (k + 1) * HD] * scale * gains[0, k : k + 1, :]).astype(BF16)
            for k in range(width // HD)
        ], axis=1)
        for d in range(n):
            sbuf[d] = normed[:, d * depth : (d + 1) * depth]
    with jax.named_scope("barrier"):
        pl.semaphore_wait(barrier, n + m - 2)

    def turn(first, last):
        for b in range(first, last, 2):
            settle(kbuf.at[pl.ds(b, 2)], ksem.at[b // 2])

        @pl.loop(first, last)
        def _(b):
            turned[b] = kbuf[b].T

    def spread(j):
        to = flip(me, j, n)
        return pltpu.make_async_remote_copy(
            src_ref=sbuf.at[to], dst_ref=rbuf.at[j], send_sem=s1, recv_sem=r1,
            device_id={"dp": to, "tensor": mt}, device_id_type=MESH)

    with jax.named_scope("spread"):
        for j in range(n - 1, 0, -1):
            spread(j).start()
        rbuf[0] = sbuf[me]

    with jax.named_scope("loadwait"):
        settle(tables, lsem.at[2])
        small[6].wait()
        small[7].wait()
        settle(w.at[:, pl.ds(0, qc)], wsem.at[0])
        settle(w.at[:, pl.ds(qc, 2 * kc)], wsem.at[1])
        wload.wait()
        for load in keys[EARLY:ready]:
            load.start()
    with jax.named_scope("rope"):
        row = lax.broadcasted_iota(jnp.int32, (rows, HD), 0)
        lane = lax.broadcasted_iota(jnp.int32, (rows, HD), 1)
        position = jnp.zeros((rows, HD), jnp.int32)
        for r in range(rows):
            position = jnp.where(row == r, pos_s[r], position)
        angles = position.astype(F32) / rope_factor * tables[2]
        cos_part = jnp.cos(angles)
        sin_part = jnp.sin(angles)
        sin_part = jnp.where(lane < HD // 2, -sin_part, sin_part)

    with jax.named_scope("turn"):
        wt[...] = wo[...].T
        turn(0, EARLY)
        for load in keys[ready:]:
            load.start()
    with jax.named_scope("spreadwait"):
        settle(rbuf.at[pl.ds(1, n - 1)], r1)
    for load in values:
        load.start()
    x = rbuf[...].reshape(n * rows, depth)

    def pair(c):
        span = pl.ds(c * chunk, chunk)
        return pltpu.make_async_remote_copy(
            src_ref=pout.at[:, :, span], dst_ref=pin.at[:, :, span], send_sem=sp, recv_sem=rp.at[c],
            device_id={"dp": flip(me, 1, n), "tensor": mt}, device_id_type=MESH)

    def give(i, c):
        span = pl.ds(c * chunk, chunk)
        return pltpu.make_async_remote_copy(
            src_ref=rs.at[i, :, span], dst_ref=rr.at[i, :, span], send_sem=s2, recv_sem=r2.at[c],
            device_id={"dp": flip(me, 2 * i, n), "tensor": mt}, device_id_type=MESH)

    with jax.named_scope("mm"):
        for c in range(chunks):
            at = slice(c * chunk, (c + 1) * chunk)
            product = jnp.dot(x, w[:, at], preferred_element_type=F32).reshape(n, rows, chunk)
            for i in range(half):
                pout[i, :, at] = product[2 * i + 1].astype(BF16)
            pair(c).start()
            for i in range(half):
                keep[i, :, at] = product[2 * i]
    with jax.named_scope("pair"):
        for c in range(chunks):
            at = slice(c * chunk, (c + 1) * chunk)
            pair(c).wait_recv()
            for i in range(half - 1, 0, -1):
                rs[i, :, at] = (keep[i, :, at] + pin[i, :, at].astype(F32)).astype(BF16)
                give(i, c).start()

    with jax.named_scope("turnkeys"):
        turn(EARLY, ready)

    def head(block, gain):
        mean = jnp.mean(block * block, axis=-1, keepdims=True)
        block = block * lax.rsqrt(mean + epsilon) * gain
        return block * cos_part + pltpu.roll(block, HD // 2, 1) * sin_part

    for c in range(chunks):
        at = slice(c * chunk, (c + 1) * chunk)
        with jax.named_scope("givewait"):
            settle(rr.at[pl.ds(1, half - 1), :, pl.ds(c * chunk, chunk)], r2.at[c])
        total = keep[0, :, at] + pin[0, :, at].astype(F32)
        for i in range(1, half):
            total = total + rr[i, :, at].astype(F32)
        for k in range(chunk // HD):
            block = total[:, k * HD : (k + 1) * HD]
            h = (c * chunk) // HD + k
            if h < heads:
                query = head(block, tables[0]) * QPRE ** (-0.5)
                q_s[:, h, :] = query.astype(BF16).astype(F32)
            elif h < heads + groups:
                g = h - heads
                key = head(block, tables[1]).astype(BF16)
                nk_out[:, g * HD : (g + 1) * HD] = key
                for r in range(per):
                    kx_s[:, g * per + r, :] = key.astype(F32)
            else:
                g = h - heads - groups
                value = block.astype(BF16)
                nv_out[:, g * HD : (g + 1) * HD] = value
                for r in range(per):
                    vx_s[:, g * per + r, :] = value.astype(F32)

    def gather(c, j):
        return pltpu.make_async_remote_copy(
            src_ref=att.at[c], dst_ref=gath.at[c, j], send_sem=s3, recv_sem=r3.at[c],
            device_id={"dp": flip(me, j, n), "tensor": mt}, device_id_type=MESH)

    middle = (m // 2 - 1, m // 2)
    quarter = n // 4
    slots = (
        [*range(quarter), *range(n - quarter, n)],
        [*range(quarter, n - quarter)],
    )

    def reduce(c, h):
        return pltpu.make_async_remote_copy(
            src_ref=ps.at[c, h], dst_ref=pr.at[c, mt], send_sem=s4, recv_sem=r4.at[c],
            device_id={"dp": me, "tensor": middle[h]}, device_id_type=MESH)

    def final(c, i, j, b):
        return pltpu.make_async_remote_copy(
            src_ref=fs.at[c, i], dst_ref=fr.at[c, me], send_sem=s5.at[b], recv_sem=r5.at[c],
            device_id={"dp": flip(me, j, n), "tensor": b}, device_id_type=MESH)

    which = lax.broadcasted_iota(jnp.int32, (heads, HD), 0) // per
    slot = lax.broadcasted_iota(jnp.int32, (heads, ctx), 1)

    def score(c):
        for b in range(c * part, (c + 1) * part):
            q8 = q_s[b]
            wide = jnp.concatenate(
                [jnp.where(which == g, q8, 0.0) for g in range(groups)], axis=1).astype(BF16)
            if b < ready:
                scores[b] = jnp.dot(wide, turned[b], preferred_element_type=F32)
            else:
                scores[b] = lax.dot_general(
                    wide, kbuf[b - ready], (((1,), (1,)), ((), ())), preferred_element_type=F32)

    def mix(c):
        for b in range(c * part, (c + 1) * part):
            own = jnp.sum(q_s[b] * kx_s[b], axis=-1, keepdims=True)
            s = jnp.where(slot < len_s[b], scores[b], -jnp.inf)
            largest = jnp.maximum(jnp.max(s, axis=-1, keepdims=True), own)
            e = jnp.exp(s - largest)
            e_own = jnp.exp(own - largest)
            sums[b] = jnp.broadcast_to(jnp.sum(e, axis=-1, keepdims=True) + e_own, (heads, HD))
            owns[b] = e_own.astype(BF16).astype(F32) * vx_s[b]
            weights[b] = e.astype(BF16)
        for b in range(c * part, (c + 1) * part):
            mixture = jnp.dot(weights[b], vbuf[b], preferred_element_type=F32)
            got = mixture[:, :HD]
            for g in range(1, groups):
                got = jnp.where(which == g, mixture[:, g * HD : (g + 1) * HD], got)
            mixed[b] = (got + owns[b]) / sums[b]
        for h in range(heads):
            att[c, :, h * HD : (h + 1) * HD] = mixed[c * part : (c + 1) * part, h, :].astype(BF16)
        for j in range(n - 1, 0, -1):
            gather(c, j).start()
        gath[c, 0] = att[c]

    def project(c):
        with jax.named_scope("gatherwait"):
            settle(gath.at[c, pl.ds(1, n - 1)], r3.at[c])
        y = lax.dot_general(
            gath[c].reshape(n * part, qc), wt[...], (((1,), (0,)), ((), ())), preferred_element_type=F32)
        y = y.astype(BF16)
        edge = quarter * part
        ps[c, 0, :edge] = y[:edge]
        ps[c, 0, edge:] = y[3 * edge :]
        ps[c, 1] = y[edge : 3 * edge]
        for h in range(2):
            @pl.when(mt != middle[h])
            def _():
                reduce(c, h).start()

    def total(c):
        for h in range(2):
            @pl.when(mt == middle[h])
            def _():
                pr[c, middle[h]] = ps[c, h]
                with jax.named_scope("reducewait"):
                    settle(pr.at[c, pl.ds(1, m - 1)], r4.at[c])
                got = pr[c, 0].astype(F32)
                for t in range(1, m):
                    got = got + pr[c, t].astype(F32)
                for i, j in enumerate(slots[h]):
                    fs[c, i] = got[i * part : (i + 1) * part].astype(BF16)
                far = sorted(range(m), key=lambda b: -abs(b - middle[h]))
                for b in far:
                    for i, j in reversed([*enumerate(slots[h])]):
                        if (j, b) == (0, middle[0]):
                            fr[c, me] = fs[c, i]
                        else:
                            final(c, i, j, b).start()

    def finish(c):
        with jax.named_scope("finalwait"):
            @pl.when(mt == middle[0])
            def _():
                settle(fr.at[c, pl.ds(0, n - 1)], r5.at[c])

            @pl.when(mt != middle[0])
            def _():
                settle(fr.at[c], r5.at[c])

        blocks = [fr[c, d].astype(F32) for d in range(n)]
        square = jnp.zeros((part, 1), F32)
        for block in blocks:
            square = square + jnp.sum(block * block, axis=-1, keepdims=True)
        factor = lax.rsqrt(square * (1.0 / width) + epsilon)
        y = jnp.concatenate(blocks, axis=1)
        mine = slice(c * part, (c + 1) * part)
        for k in range(width // HD):
            at = slice(k * HD, (k + 1) * HD)
            hid_out[mine, at] = (
                tok_v[mine, at].astype(F32) + y[:, at] * factor * gains[1, k : k + 1, :]).astype(BF16)

    def run(step, c):
        with jax.named_scope(step.__name__):
            step(c)

    with jax.named_scope("cachewait"):
        for b in range(ready, rows, 2):
            settle(kbuf.at[pl.ds(b - ready, 2)], ksem.at[b // 2])
        for b in range(0, rows, 2):
            settle(vbuf.at[pl.ds(b, 2)], vsem.at[b // 2])
    run(score, 0)
    for c in range(CHUNKS):
        if c + 1 < CHUNKS:
            run(score, c + 1)
        else:
            run(project, 0)
        run(mix, c)
    for c in range(1, CHUNKS):
        run(project, c)
    for c in range(CHUNKS):
        run(total, c)
    for c in range(CHUNKS):
        run(finish, c)

    with jax.named_scope("drain"):
        settle(rbuf.at[pl.ds(1, n - 1)], s1)
        settle(pout, sp)
        settle(rs.at[pl.ds(1, half - 1)], s2)
        settle(gath.at[:, pl.ds(1, n - 1)], s3)

        for h in range(2):
            @pl.when(mt == middle[h])
            def _():
                settle(ps.at[:, 0], s4)
                for b in range(m):
                    count = half - 1 if (h, b) == (0, middle[0]) else half
                    settle(fr.at[:, pl.ds(0, count)], s5.at[b])

        @pl.when((mt < middle[0]) | (mt > middle[1]))
        def _():
            settle(ps, s4)


def store_kernel(hid_v, nk_v, nv_v, hid_out, nk_out, nv_out, sem):
    copies = [
        pltpu.make_async_copy(hid_v, hid_out, sem.at[0]),
        pltpu.make_async_copy(nk_v, nk_out, sem.at[1]),
        pltpu.make_async_copy(nv_v, nv_out, sem.at[2]),
    ]
    for move in copies:
        move.start()
    for move in copies:
        move.wait()


def per_device(
    n, m, tokens, lengths, positions, in_gain, q_weight, k_weight, v_weight, q_gain, k_gain,
    key_cache, value_cache, out_weight, post_gain,
):
    rows, width = tokens.shape
    depth, qc = q_weight.shape
    kc = k_weight.shape[1]
    cols = qc + 2 * kc
    chunks = cols // min(512, cols)
    heads = qc // HD
    ctx = key_cache.shape[1]
    ocols = out_weight.shape[1]
    part = rows // CHUNKS
    half = n // 2
    exponent = np.arange(HD // 2) * (2.0 / HD)
    frequency = np.power(rope_base, -exponent).astype(np.float32)
    frequency = np.concatenate([frequency, frequency])[None, :]

    full = pl.BlockSpec(memory_space=VMEM)
    anywhere = pl.BlockSpec(memory_space=pltpu.HBM)
    dma = pltpu.SemaphoreType.DMA
    results = [
        jax.ShapeDtypeStruct((rows, width), BF16),
        jax.ShapeDtypeStruct((rows, kc), BF16),
        jax.ShapeDtypeStruct((rows, kc), BF16),
    ]
    made = pl.pallas_call(
        functools.partial(layer_kernel, n, m),
        name="layer",
        out_shape=results,
        in_specs=[anywhere] * 14,
        out_specs=[full] * 3,
        scratch_shapes=[
            VMEM((rows, width), BF16),
            SMEM((rows,), jnp.int32),
            SMEM((rows,), jnp.int32),
            VMEM((3, 1, HD), F32),
            VMEM((2, width // HD, HD), F32),
            VMEM((depth, cols), BF16),
            VMEM((READY, ctx, kc), BF16),
            VMEM((rows, ctx, kc), BF16),
            VMEM((READY, kc, ctx), BF16),
            VMEM((ocols, qc), BF16),
            VMEM((qc, ocols), BF16),
            VMEM((n, rows, depth), BF16),
            VMEM((n, rows, depth), BF16),
            VMEM((half, rows, cols), F32),
            VMEM((half, rows, cols), BF16),
            VMEM((half, rows, cols), BF16),
            VMEM((half, rows, cols), BF16),
            VMEM((half, rows, cols), BF16),
            VMEM((rows, heads, HD), F32),
            VMEM((rows, heads, HD), F32),
            VMEM((rows, heads, HD), F32),
            VMEM((rows, heads, ctx), F32),
            VMEM((rows, heads, ctx), BF16),
            VMEM((rows, heads, HD), F32),
            VMEM((rows, heads, HD), F32),
            VMEM((rows, heads, HD), F32),
            VMEM((CHUNKS, part, qc), BF16),
            VMEM((CHUNKS, n, part, qc), BF16),
            VMEM((CHUNKS, 2, half * part, ocols), BF16),
            VMEM((CHUNKS, m, half * part, ocols), BF16),
            VMEM((CHUNKS, half, part, ocols), BF16),
            VMEM((CHUNKS, n, part, ocols), BF16),
            dma((5,)), dma((2,)), dma((rows // 2,)), dma((rows // 2,)), dma, dma, dma, dma, dma((chunks,)), dma, dma((chunks,)),
            dma, dma((CHUNKS,)), dma, dma((CHUNKS,)), dma((m,)), dma((CHUNKS,)),
        ],
        compiler_params=pltpu.CompilerParams(
            collective_id=0, has_side_effects=True, vmem_limit_bytes=LIMIT),
    )(*[pltpu.with_memory_space_constraint(operand, pltpu.HBM) for operand in (
        tokens, lengths, positions, jnp.asarray(frequency), in_gain.reshape(width // HD, HD),
        q_weight, k_weight, v_weight, q_gain[None, :], k_gain[None, :],
        key_cache, value_cache, out_weight.T, post_gain.reshape(width // HD, HD))])
    return pl.pallas_call(
        store_kernel,
        name="store",
        out_shape=results,
        in_specs=[full] * 3,
        out_specs=[anywhere] * 3,
        scratch_shapes=[dma((3,))],
        compiler_params=pltpu.CompilerParams(vmem_limit_bytes=1 << 20),
    )(*made)


def solution(mesh):
    n, m = mesh.shape["dp"], mesh.shape["tensor"]
    return jax.shard_map(
        functools.partial(per_device, n, m),
        mesh=mesh,
        in_specs=(
            P("dp", None),
            P("dp"),
            P("dp"),
            P(),
            P("dp", "tensor"),
            P("dp", "tensor"),
            P("dp", "tensor"),
            P(),
            P(),
            P("dp", None, "tensor"),
            P("dp", None, "tensor"),
            P("tensor", "dp"),
            P(),
        ),
        out_specs=(P("dp", None), P("dp", "tensor"), P("dp", "tensor")),
        check_vma=False,
    )
```

```python
import functools

import jax
import jax.numpy as jnp
import numpy as np
from jax import lax
from jax.experimental import pallas as pl
from jax.experimental.pallas import tpu as pltpu
from jax.sharding import PartitionSpec as P

HD = 128
QPRE = 168
LIMIT = 54000000
CHUNKS = 4
EARLY = 4
READY = 12

epsilon = 1e-06
rope_base = 1000000.0
rope_factor = 8.0

MESH = pl.DeviceIdType.MESH
VMEM = pltpu.VMEM
SMEM = pltpu.SMEM
F32 = jnp.float32
BF16 = jnp.bfloat16


def flip(a, b, n):
    total, bit = 0, 1
    while bit < n:
        total = total + lax.rem(a // bit + b // bit, 2) * bit
        bit *= 2
    return total


def layer_kernel(
    n, m, tok_hbm, len_hbm, pos_hbm, freq_hbm, gain_hbm, wq_hbm, wk_hbm, wv_hbm, qg_hbm, kg_hbm,
    kc_hbm, vc_hbm, wo_hbm, post_hbm,
    hid_out, nk_out, nv_out,
    tok_v, len_s, pos_s, tables, gains, w, kbuf, vbuf, turned, wo, wt,
    sbuf, rbuf, keep, pout, pin, rs, rr, q_s, kx_s, vx_s, scores, weights, sums, owns, mixed,
    att, gath, ps, pr, fs, fr,
    lsem, wsem, ksem, vsem, osem, s1, r1, sp, rp, s2, r2, s3, r3, s4, r4, s5, r5,
):
    me = lax.axis_index("dp")
    mt = lax.axis_index("tensor")
    rows, width = tok_v.shape
    depth, cols = w.shape
    qc, kc = wq_hbm.shape[1], wk_hbm.shape[1]
    ctx = kbuf.shape[1]
    ocols = wo.shape[0]
    heads, groups = qc // HD, kc // HD
    per = heads // groups
    half = n // 2
    part = rows // CHUNKS
    ready = turned.shape[0]
    chunk = min(512, cols)
    chunks = cols // chunk

    barrier = pltpu.get_barrier_semaphore()
    for a in range(1, n):
        pl.semaphore_signal(
            barrier, inc=1, device_id={"dp": lax.rem(me + a, n), "tensor": mt}, device_id_type=MESH)
    for b in range(1, m):
        pl.semaphore_signal(
            barrier, inc=1, device_id={"dp": me, "tensor": lax.rem(mt + b, m)}, device_id_type=MESH)

    copy = pltpu.make_async_copy
    small = [
        copy(tok_hbm, tok_v, lsem.at[0]),
        copy(gain_hbm, gains.at[0], lsem.at[1]),
        copy(post_hbm, gains.at[1], lsem.at[1]),
        copy(qg_hbm, tables.at[0], lsem.at[2]),
        copy(kg_hbm, tables.at[1], lsem.at[2]),
        copy(freq_hbm, tables.at[2], lsem.at[2]),
        copy(len_hbm, len_s, lsem.at[3]),
        copy(pos_hbm, pos_s, lsem.at[4]),
    ]
    loads = [
        copy(wq_hbm, w.at[:, pl.ds(0, qc)], wsem.at[0]),
        copy(wk_hbm, w.at[:, pl.ds(qc, kc)], wsem.at[1]),
        copy(wv_hbm, w.at[:, pl.ds(qc + kc, kc)], wsem.at[1]),
    ]
    keys = [copy(kc_hbm.at[b], kbuf.at[b % ready], ksem.at[b // part]) for b in range(rows)]
    values = [copy(vc_hbm.at[b], vbuf.at[b], vsem.at[b // part]) for b in range(rows)]

    def settle(ref, sem):
        copy(ref, ref, sem).wait()

    wload = copy(wo_hbm, wo, osem)
    for load in small + loads + [wload]:
        load.start()

    with jax.named_scope("norm"):
        with jax.named_scope("tokwait"):
            settle(tok_v, lsem.at[0])
        settle(gains, lsem.at[1])
        for load in keys[:EARLY]:
            load.start()
        tok = tok_v[...].astype(F32)
        scale = lax.rsqrt(jnp.sum(tok * tok, axis=-1, keepdims=True) * (1.0 / width) + epsilon)
        normed = jnp.concatenate([
            (tok[:, k * HD : (k + 1) * HD] * scale * gains[0, k : k + 1, :]).astype(BF16)
            for k in range(width // HD)
        ], axis=1)
        for d in range(n):
            sbuf[d] = normed[:, d * depth : (d + 1) * depth]
    with jax.named_scope("barrier"):
        pl.semaphore_wait(barrier, n + m - 2)

    def turn(first, last):
        for b in range(first, last, part):
            settle(kbuf.at[pl.ds(b, part)], ksem.at[b // part])

        @pl.loop(first, last)
        def _(b):
            turned[b] = kbuf[b].T

    def spread(j):
        to = flip(me, j, n)
        return pltpu.make_async_remote_copy(
            src_ref=sbuf.at[to], dst_ref=rbuf.at[j], send_sem=s1, recv_sem=r1,
            device_id={"dp": to, "tensor": mt}, device_id_type=MESH)

    with jax.named_scope("spread"):
        for j in range(n - 1, 0, -1):
            spread(j).start()
        rbuf[0] = sbuf[me]

    with jax.named_scope("loadwait"):
        settle(tables, lsem.at[2])
        small[6].wait()
        small[7].wait()
        settle(w.at[:, pl.ds(0, qc)], wsem.at[0])
        settle(w.at[:, pl.ds(qc, 2 * kc)], wsem.at[1])
        wload.wait()
        for load in keys[EARLY:ready]:
            load.start()
    with jax.named_scope("rope"):
        row = lax.broadcasted_iota(jnp.int32, (rows, HD), 0)
        lane = lax.broadcasted_iota(jnp.int32, (rows, HD), 1)
        position = jnp.zeros((rows, HD), jnp.int32)
        for r in range(rows):
            position = jnp.where(row == r, pos_s[r], position)
        angles = position.astype(F32) / rope_factor * tables[2]
        cos_part = jnp.cos(angles)
        sin_part = jnp.sin(angles)
        sin_part = jnp.where(lane < HD // 2, -sin_part, sin_part)

    with jax.named_scope("turn"):
        wt[...] = wo[...].T
        turn(0, EARLY)
        for load in keys[ready:]:
            load.start()
    with jax.named_scope("spreadwait"):
        settle(rbuf.at[pl.ds(1, n - 1)], r1)
    for load in values:
        load.start()
    x = rbuf[...].reshape(n * rows, depth)

    def pair(c):
        span = pl.ds(c * chunk, chunk)
        return pltpu.make_async_remote_copy(
            src_ref=pout.at[:, :, span], dst_ref=pin.at[:, :, span], send_sem=sp, recv_sem=rp.at[c],
            device_id={"dp": flip(me, 1, n), "tensor": mt}, device_id_type=MESH)

    def give(i, c):
        span = pl.ds(c * chunk, chunk)
        return pltpu.make_async_remote_copy(
            src_ref=rs.at[i, :, span], dst_ref=rr.at[i, :, span], send_sem=s2, recv_sem=r2.at[c],
            device_id={"dp": flip(me, 2 * i, n), "tensor": mt}, device_id_type=MESH)

    with jax.named_scope("mm"):
        for c in range(chunks):
            at = slice(c * chunk, (c + 1) * chunk)
            product = jnp.dot(x, w[:, at], preferred_element_type=F32).reshape(n, rows, chunk)
            for i in range(half):
                pout[i, :, at] = product[2 * i + 1].astype(BF16)
            pair(c).start()
            for i in range(half):
                keep[i, :, at] = product[2 * i]
    with jax.named_scope("pair"):
        for c in range(chunks):
            at = slice(c * chunk, (c + 1) * chunk)
            pair(c).wait_recv()
            for i in range(half - 1, 0, -1):
                rs[i, :, at] = (keep[i, :, at] + pin[i, :, at].astype(F32)).astype(BF16)
                give(i, c).start()

    with jax.named_scope("turnkeys"):
        turn(EARLY, ready)

    def head(block, gain):
        mean = jnp.mean(block * block, axis=-1, keepdims=True)
        block = block * lax.rsqrt(mean + epsilon) * gain
        return block * cos_part + pltpu.roll(block, HD // 2, 1) * sin_part

    def split(c):
        at = slice(c * chunk, (c + 1) * chunk)
        with jax.named_scope("givewait"):
            settle(rr.at[pl.ds(1, half - 1), :, pl.ds(c * chunk, chunk)], r2.at[c])
        total = keep[0, :, at] + pin[0, :, at].astype(F32)
        for i in range(1, half):
            total = total + rr[i, :, at].astype(F32)
        for k in range(chunk // HD):
            block = total[:, k * HD : (k + 1) * HD]
            h = (c * chunk) // HD + k
            if h < heads:
                query = head(block, tables[0]) * QPRE ** (-0.5)
                q_s[:, h, :] = query.astype(BF16).astype(F32)
            elif h < heads + groups:
                g = h - heads
                key = head(block, tables[1]).astype(BF16)
                nk_out[:, g * HD : (g + 1) * HD] = key
                for r in range(per):
                    kx_s[:, g * per + r, :] = key.astype(F32)
            else:
                g = h - heads - groups
                value = block.astype(BF16)
                nv_out[:, g * HD : (g + 1) * HD] = value
                for r in range(per):
                    vx_s[:, g * per + r, :] = value.astype(F32)

    def gather(c, j):
        return pltpu.make_async_remote_copy(
            src_ref=att.at[c], dst_ref=gath.at[c, j], send_sem=s3, recv_sem=r3.at[c],
            device_id={"dp": flip(me, j, n), "tensor": mt}, device_id_type=MESH)

    middle = (m // 2 - 1, m // 2)
    quarter = n // 4
    slots = (
        [*range(quarter), *range(n - quarter, n)],
        [*range(quarter, n - quarter)],
    )

    def reduce(c, h):
        return pltpu.make_async_remote_copy(
            src_ref=ps.at[c, h], dst_ref=pr.at[c, mt], send_sem=s4, recv_sem=r4.at[c],
            device_id={"dp": me, "tensor": middle[h]}, device_id_type=MESH)

    def final(c, i, j, b):
        return pltpu.make_async_remote_copy(
            src_ref=fs.at[c, i], dst_ref=fr.at[c, me], send_sem=s5.at[b], recv_sem=r5.at[c],
            device_id={"dp": flip(me, j, n), "tensor": b}, device_id_type=MESH)

    which = lax.broadcasted_iota(jnp.int32, (heads, HD), 0) // per
    slot = lax.broadcasted_iota(jnp.int32, (heads, ctx), 1)

    some = chunk // HD
    wide = some // per * HD

    def score(c, p):
        for b in range(c * part, (c + 1) * part):
            q = q_s[b, p * some : (p + 1) * some, :]
            q = jnp.concatenate(
                [jnp.where(which[:some] == g, q, 0.0) for g in range(some // per)], axis=1).astype(BF16)
            at = slice(p * wide, (p + 1) * wide)
            if b < ready:
                got = jnp.dot(q, turned[b, at, :], preferred_element_type=F32)
            else:
                got = lax.dot_general(
                    q, kbuf[b - ready, :, at], (((1,), (1,)), ((), ())), preferred_element_type=F32)
            scores[b, p * some : (p + 1) * some, :] = got

    def soft(c):
        for b in range(c * part, (c + 1) * part):
            own = jnp.sum(q_s[b] * kx_s[b], axis=-1, keepdims=True)
            s = jnp.where(slot < len_s[b], scores[b], -jnp.inf)
            largest = jnp.maximum(jnp.max(s, axis=-1, keepdims=True), own)
            e = jnp.exp(s - largest)
            e_own = jnp.exp(own - largest)
            sums[b] = jnp.broadcast_to(jnp.sum(e, axis=-1, keepdims=True) + e_own, (heads, HD))
            owns[b] = e_own.astype(BF16).astype(F32) * vx_s[b]
            weights[b] = e.astype(BF16)

    def mix(c):
        for b in range(c * part, (c + 1) * part):
            mixture = jnp.dot(weights[b], vbuf[b], preferred_element_type=F32)
            got = mixture[:, :HD]
            for g in range(1, groups):
                got = jnp.where(which == g, mixture[:, g * HD : (g + 1) * HD], got)
            mixed[b] = (got + owns[b]) / sums[b]
        for h in range(heads):
            att[c, :, h * HD : (h + 1) * HD] = mixed[c * part : (c + 1) * part, h, :].astype(BF16)
        for j in range(n - 1, 0, -1):
            gather(c, j).start()
        gath[c, 0] = att[c]

    def project(c):
        with jax.named_scope("gatherwait"):
            settle(gath.at[c, pl.ds(1, n - 1)], r3.at[c])
        y = lax.dot_general(
            gath[c].reshape(n * part, qc), wt[...], (((1,), (0,)), ((), ())), preferred_element_type=F32)
        y = y.astype(BF16)
        edge = quarter * part
        ps[c, 0, :edge] = y[:edge]
        ps[c, 0, edge:] = y[3 * edge :]
        ps[c, 1] = y[edge : 3 * edge]
        for h in range(2):
            @pl.when(mt != middle[h])
            def _():
                reduce(c, h).start()

    def total(c):
        for h in range(2):
            @pl.when(mt == middle[h])
            def _():
                pr[c, middle[h]] = ps[c, h]
                with jax.named_scope("reducewait"):
                    settle(pr.at[c, pl.ds(1, m - 1)], r4.at[c])
                got = pr[c, 0].astype(F32)
                for t in range(1, m):
                    got = got + pr[c, t].astype(F32)
                for i, j in enumerate(slots[h]):
                    fs[c, i] = got[i * part : (i + 1) * part].astype(BF16)
                far = sorted(range(m), key=lambda b: -abs(b - middle[h]))
                for b in far:
                    for i, j in reversed([*enumerate(slots[h])]):
                        if (j, b) == (0, middle[0]):
                            fr[c, me] = fs[c, i]
                        else:
                            final(c, i, j, b).start()

    def finish(c):
        with jax.named_scope("finalwait"):
            @pl.when(mt == middle[0])
            def _():
                settle(fr.at[c, pl.ds(0, n - 1)], r5.at[c])

            @pl.when(mt != middle[0])
            def _():
                settle(fr.at[c], r5.at[c])

        blocks = [fr[c, d].astype(F32) for d in range(n)]
        square = jnp.zeros((part, 1), F32)
        for block in blocks:
            square = square + jnp.sum(block * block, axis=-1, keepdims=True)
        factor = lax.rsqrt(square * (1.0 / width) + epsilon)
        y = jnp.concatenate(blocks, axis=1)
        mine = slice(c * part, (c + 1) * part)
        for k in range(width // HD):
            at = slice(k * HD, (k + 1) * HD)
            hid_out[mine, at] = (
                tok_v[mine, at].astype(F32) + y[:, at] * factor * gains[1, k : k + 1, :]).astype(BF16)

    def run(step, *which):
        with jax.named_scope(step.__name__):
            step(*which)

    lead = qc // chunk
    with jax.named_scope("cachewait"):
        for b in range(ready, rows, part):
            settle(kbuf.at[pl.ds(b - ready, part)], ksem.at[b // part])
    for p in range(lead):
        run(split, p)
        for c in range(2):
            run(score, c, p)
    for c in range(lead, chunks):
        run(split, c)
    with jax.named_scope("valueswait"):
        for b in range(0, rows, part):
            settle(vbuf.at[pl.ds(b, part)], vsem.at[b // part])
    for c in range(CHUNKS):
        if 0 < c < CHUNKS - 1:
            for p in range(lead):
                run(score, c + 1, p)
        run(soft, c)
        run(mix, c)
    run(project, 0)
    for c in range(1, CHUNKS):
        run(project, c)
    for c in range(CHUNKS):
        run(total, c)
    for c in range(CHUNKS):
        run(finish, c)

    with jax.named_scope("drain"):
        settle(rbuf.at[pl.ds(1, n - 1)], s1)
        settle(pout, sp)
        settle(rs.at[pl.ds(1, half - 1)], s2)
        settle(gath.at[:, pl.ds(1, n - 1)], s3)

        for h in range(2):
            @pl.when(mt == middle[h])
            def _():
                settle(ps.at[:, 0], s4)
                for b in range(m):
                    count = half - 1 if (h, b) == (0, middle[0]) else half
                    settle(fr.at[:, pl.ds(0, count)], s5.at[b])

        @pl.when((mt < middle[0]) | (mt > middle[1]))
        def _():
            settle(ps, s4)


def store_kernel(hid_v, nk_v, nv_v, hid_out, nk_out, nv_out, sem):
    copies = [
        pltpu.make_async_copy(hid_v, hid_out, sem.at[0]),
        pltpu.make_async_copy(nk_v, nk_out, sem.at[1]),
        pltpu.make_async_copy(nv_v, nv_out, sem.at[2]),
    ]
    for move in copies:
        move.start()
    for move in copies:
        move.wait()


def per_device(
    n, m, tokens, lengths, positions, in_gain, q_weight, k_weight, v_weight, q_gain, k_gain,
    key_cache, value_cache, out_weight, post_gain,
):
    rows, width = tokens.shape
    depth, qc = q_weight.shape
    kc = k_weight.shape[1]
    cols = qc + 2 * kc
    chunks = cols // min(512, cols)
    heads = qc // HD
    ctx = key_cache.shape[1]
    ocols = out_weight.shape[1]
    part = rows // CHUNKS
    half = n // 2
    exponent = np.arange(HD // 2) * (2.0 / HD)
    frequency = np.power(rope_base, -exponent).astype(np.float32)
    frequency = np.concatenate([frequency, frequency])[None, :]

    full = pl.BlockSpec(memory_space=VMEM)
    anywhere = pl.BlockSpec(memory_space=pltpu.HBM)
    dma = pltpu.SemaphoreType.DMA
    results = [
        jax.ShapeDtypeStruct((rows, width), BF16),
        jax.ShapeDtypeStruct((rows, kc), BF16),
        jax.ShapeDtypeStruct((rows, kc), BF16),
    ]
    made = pl.pallas_call(
        functools.partial(layer_kernel, n, m),
        name="layer",
        out_shape=results,
        in_specs=[anywhere] * 14,
        out_specs=[full] * 3,
        scratch_shapes=[
            VMEM((rows, width), BF16),
            SMEM((rows,), jnp.int32),
            SMEM((rows,), jnp.int32),
            VMEM((3, 1, HD), F32),
            VMEM((2, width // HD, HD), F32),
            VMEM((depth, cols), BF16),
            VMEM((READY, ctx, kc), BF16),
            VMEM((rows, ctx, kc), BF16),
            VMEM((READY, kc, ctx), BF16),
            VMEM((ocols, qc), BF16),
            VMEM((qc, ocols), BF16),
            VMEM((n, rows, depth), BF16),
            VMEM((n, rows, depth), BF16),
            VMEM((half, rows, cols), F32),
            VMEM((half, rows, cols), BF16),
            VMEM((half, rows, cols), BF16),
            VMEM((half, rows, cols), BF16),
            VMEM((half, rows, cols), BF16),
            VMEM((rows, heads, HD), F32),
            VMEM((rows, heads, HD), F32),
            VMEM((rows, heads, HD), F32),
            VMEM((rows, heads, ctx), F32),
            VMEM((rows, heads, ctx), BF16),
            VMEM((rows, heads, HD), F32),
            VMEM((rows, heads, HD), F32),
            VMEM((rows, heads, HD), F32),
            VMEM((CHUNKS, part, qc), BF16),
            VMEM((CHUNKS, n, part, qc), BF16),
            VMEM((CHUNKS, 2, half * part, ocols), BF16),
            VMEM((CHUNKS, m, half * part, ocols), BF16),
            VMEM((CHUNKS, half, part, ocols), BF16),
            VMEM((CHUNKS, n, part, ocols), BF16),
            dma((5,)), dma((2,)), dma((CHUNKS,)), dma((CHUNKS,)), dma, dma, dma, dma, dma((chunks,)), dma, dma((chunks,)),
            dma, dma((CHUNKS,)), dma, dma((CHUNKS,)), dma((m,)), dma((CHUNKS,)),
        ],
        compiler_params=pltpu.CompilerParams(
            collective_id=0, has_side_effects=True, vmem_limit_bytes=LIMIT),
    )(*[pltpu.with_memory_space_constraint(operand, pltpu.HBM) for operand in (
        tokens, lengths, positions, jnp.asarray(frequency), in_gain.reshape(width // HD, HD),
        q_weight, k_weight, v_weight, q_gain[None, :], k_gain[None, :],
        key_cache, value_cache, out_weight.T, post_gain.reshape(width // HD, HD))])
    return pl.pallas_call(
        store_kernel,
        name="store",
        out_shape=results,
        in_specs=[full] * 3,
        out_specs=[anywhere] * 3,
        scratch_shapes=[dma((3,))],
        compiler_params=pltpu.CompilerParams(vmem_limit_bytes=1 << 20),
    )(*made)


def solution(mesh):
    n, m = mesh.shape["dp"], mesh.shape["tensor"]
    return jax.shard_map(
        functools.partial(per_device, n, m),
        mesh=mesh,
        in_specs=(
            P("dp", None),
            P("dp"),
            P("dp"),
            P(),
            P("dp", "tensor"),
            P("dp", "tensor"),
            P("dp", "tensor"),
            P(),
            P(),
            P("dp", None, "tensor"),
            P("dp", None, "tensor"),
            P("tensor", "dp"),
            P(),
        ),
        out_specs=(P("dp", None), P("dp", "tensor"), P("dp", "tensor")),
        check_vma=False,
    )
```

```python
import functools

import jax
import jax.numpy as jnp
import numpy as np
from jax import lax
from jax.experimental import pallas as pl
from jax.experimental.pallas import tpu as pltpu
from jax.sharding import PartitionSpec as P

HD = 128
QPRE = 168
LIMIT = 54000000
CHUNKS = 4
EARLY = 4
READY = 12

epsilon = 1e-06
rope_base = 1000000.0
rope_factor = 8.0

MESH = pl.DeviceIdType.MESH
VMEM = pltpu.VMEM
SMEM = pltpu.SMEM
F32 = jnp.float32
BF16 = jnp.bfloat16


def flip(a, b, n):
    total, bit = 0, 1
    while bit < n:
        total = total + lax.rem(a // bit + b // bit, 2) * bit
        bit *= 2
    return total


def layer_kernel(
    n, m, tok_hbm, len_hbm, pos_hbm, freq_hbm, gain_hbm, wq_hbm, wk_hbm, wv_hbm, qg_hbm, kg_hbm,
    kc_hbm, vc_hbm, wo_hbm, post_hbm,
    hid_out, nk_out, nv_out,
    tok_v, len_s, pos_s, tables, gains, w, kbuf, vbuf, turned, wo, wt,
    sbuf, rbuf, keep, pout, pin, rs, rr, q_s, kx_s, vx_s, scores, weights, sums, owns, mixed,
    att, gath, ps, pr, fs, fr,
    lsem, wsem, ksem, vsem, osem, s1, r1, sp, rp, s2, r2, s3, r3, s4, r4, s5, r5,
):
    me = lax.axis_index("dp")
    mt = lax.axis_index("tensor")
    rows, width = tok_v.shape
    depth, cols = w.shape
    qc, kc = wq_hbm.shape[1], wk_hbm.shape[1]
    ctx = kbuf.shape[1]
    ocols = wo.shape[0]
    heads, groups = qc // HD, kc // HD
    per = heads // groups
    half = n // 2
    part = rows // CHUNKS
    ready = turned.shape[0]
    chunk = min(512, cols)
    chunks = cols // chunk

    barrier = pltpu.get_barrier_semaphore()
    for a in range(1, n):
        pl.semaphore_signal(
            barrier, inc=1, device_id={"dp": lax.rem(me + a, n), "tensor": mt}, device_id_type=MESH)
    for b in range(1, m):
        pl.semaphore_signal(
            barrier, inc=1, device_id={"dp": me, "tensor": lax.rem(mt + b, m)}, device_id_type=MESH)

    copy = pltpu.make_async_copy
    small = [
        copy(tok_hbm, tok_v, lsem.at[0]),
        copy(gain_hbm, gains.at[0], lsem.at[1]),
        copy(post_hbm, gains.at[1], lsem.at[1]),
        copy(qg_hbm, tables.at[0], lsem.at[2]),
        copy(kg_hbm, tables.at[1], lsem.at[2]),
        copy(freq_hbm, tables.at[2], lsem.at[2]),
        copy(len_hbm, len_s, lsem.at[3]),
        copy(pos_hbm, pos_s, lsem.at[4]),
    ]
    loads = [
        copy(wq_hbm, w.at[:, pl.ds(0, qc)], wsem.at[0]),
        copy(wk_hbm, w.at[:, pl.ds(qc, kc)], wsem.at[1]),
        copy(wv_hbm, w.at[:, pl.ds(qc + kc, kc)], wsem.at[1]),
    ]
    keys = [copy(kc_hbm.at[b], kbuf.at[b % ready], ksem.at[b // part]) for b in range(rows)]
    values = [copy(vc_hbm.at[b], vbuf.at[b], vsem.at[b // part]) for b in range(rows)]

    def settle(ref, sem):
        copy(ref, ref, sem).wait()

    wload = copy(wo_hbm, wo, osem)
    for load in small + loads + [wload]:
        load.start()

    with jax.named_scope("norm"):
        with jax.named_scope("tokwait"):
            settle(tok_v, lsem.at[0])
        settle(gains, lsem.at[1])
        for load in keys[:EARLY]:
            load.start()
        tok = tok_v[...].astype(F32)
        scale = lax.rsqrt(jnp.sum(tok * tok, axis=-1, keepdims=True) * (1.0 / width) + epsilon)
        normed = jnp.concatenate([
            (tok[:, k * HD : (k + 1) * HD] * scale * gains[0, k : k + 1, :]).astype(BF16)
            for k in range(width // HD)
        ], axis=1)
        for d in range(n):
            sbuf[d] = normed[:, d * depth : (d + 1) * depth]
    with jax.named_scope("barrier"):
        pl.semaphore_wait(barrier, n + m - 2)

    def turn(first, last):
        for b in range(first, last, part):
            settle(kbuf.at[pl.ds(b, part)], ksem.at[b // part])

        @pl.loop(first, last)
        def _(b):
            turned[b] = kbuf[b].T

    def spread(j):
        to = flip(me, j, n)
        return pltpu.make_async_remote_copy(
            src_ref=sbuf.at[to], dst_ref=rbuf.at[j], send_sem=s1, recv_sem=r1,
            device_id={"dp": to, "tensor": mt}, device_id_type=MESH)

    with jax.named_scope("spread"):
        for j in range(n - 1, 0, -1):
            spread(j).start()
        rbuf[0] = sbuf[me]

    with jax.named_scope("loadwait"):
        settle(tables, lsem.at[2])
        small[6].wait()
        small[7].wait()
        settle(w.at[:, pl.ds(0, qc)], wsem.at[0])
        settle(w.at[:, pl.ds(qc, 2 * kc)], wsem.at[1])
        wload.wait()
        for load in keys[EARLY:ready]:
            load.start()
    with jax.named_scope("rope"):
        row = lax.broadcasted_iota(jnp.int32, (rows, HD), 0)
        lane = lax.broadcasted_iota(jnp.int32, (rows, HD), 1)
        position = jnp.zeros((rows, HD), jnp.int32)
        for r in range(rows):
            position = jnp.where(row == r, pos_s[r], position)
        angles = position.astype(F32) / rope_factor * tables[2]
        cos_part = jnp.cos(angles)
        sin_part = jnp.sin(angles)
        sin_part = jnp.where(lane < HD // 2, -sin_part, sin_part)

    with jax.named_scope("turn"):
        wt[...] = wo[...].T
        turn(0, EARLY)
        for load in keys[ready:]:
            load.start()
    with jax.named_scope("spreadwait"):
        settle(rbuf.at[pl.ds(1, n - 1)], r1)
    for load in values:
        load.start()
    x = rbuf[...].reshape(n * rows, depth)

    def pair(c):
        span = pl.ds(c * chunk, chunk)
        return pltpu.make_async_remote_copy(
            src_ref=pout.at[:, :, span], dst_ref=pin.at[:, :, span], send_sem=sp, recv_sem=rp.at[c],
            device_id={"dp": flip(me, 1, n), "tensor": mt}, device_id_type=MESH)

    def give(i, c):
        span = pl.ds(c * chunk, chunk)
        return pltpu.make_async_remote_copy(
            src_ref=rs.at[i, :, span], dst_ref=rr.at[i, :, span], send_sem=s2, recv_sem=r2.at[c],
            device_id={"dp": flip(me, 2 * i, n), "tensor": mt}, device_id_type=MESH)

    with jax.named_scope("mm"):
        for c in range(chunks):
            at = slice(c * chunk, (c + 1) * chunk)
            product = jnp.dot(x, w[:, at], preferred_element_type=F32).reshape(n, rows, chunk)
            for i in range(half):
                pout[i, :, at] = product[2 * i + 1].astype(BF16)
            pair(c).start()
            for i in range(half):
                keep[i, :, at] = product[2 * i]
    with jax.named_scope("pair"):
        for c in range(chunks):
            at = slice(c * chunk, (c + 1) * chunk)
            pair(c).wait_recv()
            for i in range(half - 1, 0, -1):
                rs[i, :, at] = (keep[i, :, at] + pin[i, :, at].astype(F32)).astype(BF16)
                give(i, c).start()

    with jax.named_scope("turnkeys"):
        turn(EARLY, ready)

    def head(block, gain):
        mean = jnp.mean(block * block, axis=-1, keepdims=True)
        block = block * lax.rsqrt(mean + epsilon) * gain
        return block * cos_part + pltpu.roll(block, HD // 2, 1) * sin_part

    def split(c):
        at = slice(c * chunk, (c + 1) * chunk)
        with jax.named_scope("givewait"):
            settle(rr.at[pl.ds(1, half - 1), :, pl.ds(c * chunk, chunk)], r2.at[c])
        total = keep[0, :, at] + pin[0, :, at].astype(F32)
        for i in range(1, half):
            total = total + rr[i, :, at].astype(F32)
        for k in range(chunk // HD):
            block = total[:, k * HD : (k + 1) * HD]
            h = (c * chunk) // HD + k
            if h < heads:
                query = head(block, tables[0]) * QPRE ** (-0.5)
                q_s[:, h, :] = query.astype(BF16).astype(F32)
            elif h < heads + groups:
                g = h - heads
                key = head(block, tables[1]).astype(BF16)
                nk_out[:, g * HD : (g + 1) * HD] = key
                kx_s[:, g, :] = key.astype(F32)
            else:
                g = h - heads - groups
                value = block.astype(BF16)
                nv_out[:, g * HD : (g + 1) * HD] = value
                vx_s[:, g, :] = value.astype(F32)

    def gather(c, j):
        return pltpu.make_async_remote_copy(
            src_ref=att.at[c], dst_ref=gath.at[c, j], send_sem=s3, recv_sem=r3.at[c],
            device_id={"dp": flip(me, j, n), "tensor": mt}, device_id_type=MESH)

    middle = (m // 2 - 1, m // 2)
    quarter = n // 4
    slots = (
        [*range(quarter), *range(n - quarter, n)],
        [*range(quarter, n - quarter)],
    )

    def reduce(c, h):
        return pltpu.make_async_remote_copy(
            src_ref=ps.at[c, h], dst_ref=pr.at[c, mt], send_sem=s4, recv_sem=r4.at[c],
            device_id={"dp": me, "tensor": middle[h]}, device_id_type=MESH)

    def final(c, i, j, b):
        return pltpu.make_async_remote_copy(
            src_ref=fs.at[c, i], dst_ref=fr.at[c, me], send_sem=s5.at[b], recv_sem=r5.at[c],
            device_id={"dp": flip(me, j, n), "tensor": b}, device_id_type=MESH)

    which = lax.broadcasted_iota(jnp.int32, (heads, HD), 0) // per
    slot = lax.broadcasted_iota(jnp.int32, (heads, ctx), 1)

    some = chunk // HD
    wide = some // per * HD

    def score(c, p):
        for b in range(c * part, (c + 1) * part):
            q = q_s[b, p * some : (p + 1) * some, :]
            q = jnp.concatenate(
                [jnp.where(which[:some] == g, q, 0.0) for g in range(some // per)], axis=1).astype(BF16)
            at = slice(p * wide, (p + 1) * wide)
            if b < ready:
                got = jnp.dot(q, turned[b, at, :], preferred_element_type=F32)
            else:
                got = lax.dot_general(
                    q, kbuf[b - ready, :, at], (((1,), (1,)), ((), ())), preferred_element_type=F32)
            scores[b, p * some : (p + 1) * some, :] = got

    def soft(c):
        for b in range(c * part, (c + 1) * part):
            new_key = jnp.repeat(kx_s[b], per, axis=0)
            own = jnp.sum(q_s[b] * new_key, axis=-1, keepdims=True)
            s = jnp.where(slot < len_s[b], scores[b], -jnp.inf)
            largest = jnp.maximum(jnp.max(s, axis=-1, keepdims=True), own)
            e = jnp.exp(s - largest)
            e_own = jnp.exp(own - largest)
            sums[b] = jnp.broadcast_to(jnp.sum(e, axis=-1, keepdims=True) + e_own, (heads, HD))
            owns[b] = e_own.astype(BF16).astype(F32) * jnp.repeat(vx_s[b], per, axis=0)
            weights[b] = e.astype(BF16)

    def mix(c):
        for b in range(c * part, (c + 1) * part):
            mixture = jnp.dot(weights[b], vbuf[b], preferred_element_type=F32)
            got = mixture[:, :HD]
            for g in range(1, groups):
                got = jnp.where(which == g, mixture[:, g * HD : (g + 1) * HD], got)
            mixed[b] = (got + owns[b]) / sums[b]
        for h in range(heads):
            att[c, :, h * HD : (h + 1) * HD] = mixed[c * part : (c + 1) * part, h, :].astype(BF16)
        for j in range(n - 1, 0, -1):
            gather(c, j).start()
        gath[c, 0] = att[c]

    def project(c):
        with jax.named_scope("gatherwait"):
            settle(gath.at[c, pl.ds(1, n - 1)], r3.at[c])
        y = lax.dot_general(
            gath[c].reshape(n * part, qc), wt[...], (((1,), (0,)), ((), ())), preferred_element_type=F32)
        y = y.astype(BF16)
        edge = quarter * part
        ps[c, 0, :edge] = y[:edge]
        ps[c, 0, edge:] = y[3 * edge :]
        ps[c, 1] = y[edge : 3 * edge]
        @pl.when(mt <= middle[0])
        def _():
            reduce(c, 1).start()

        @pl.when((mt < middle[0]) | (mt > middle[0]))
        def _():
            reduce(c, 0).start()

        @pl.when(mt > middle[1])
        def _():
            reduce(c, 1).start()

    def total(c):
        for h in range(2):
            @pl.when(mt == middle[h])
            def _():
                pr[c, middle[h]] = ps[c, h]
                with jax.named_scope("reducewait"):
                    settle(pr.at[c, pl.ds(1, m - 1)], r4.at[c])
                got = pr[c, 0].astype(F32)
                for t in range(1, m):
                    got = got + pr[c, t].astype(F32)
                for i, j in enumerate(slots[h]):
                    fs[c, i] = got[i * part : (i + 1) * part].astype(BF16)
                far = sorted(range(m), key=lambda b: -abs(b - middle[h]))
                for b in far:
                    for i, j in reversed([*enumerate(slots[h])]):
                        if (j, b) == (0, middle[0]):
                            fr[c, me] = fs[c, i]
                        else:
                            final(c, i, j, b).start()

    def finish(c):
        with jax.named_scope("finalwait"):
            @pl.when(mt == middle[0])
            def _():
                settle(fr.at[c, pl.ds(0, n - 1)], r5.at[c])

            @pl.when(mt != middle[0])
            def _():
                settle(fr.at[c], r5.at[c])

        blocks = [fr[c, d].astype(F32) for d in range(n)]
        square = jnp.zeros((part, 1), F32)
        for block in blocks:
            square = square + jnp.sum(block * block, axis=-1, keepdims=True)
        factor = lax.rsqrt(square * (1.0 / width) + epsilon)
        y = jnp.concatenate(blocks, axis=1)
        mine = slice(c * part, (c + 1) * part)
        for k in range(width // HD):
            at = slice(k * HD, (k + 1) * HD)
            hid_out[mine, at] = (
                tok_v[mine, at].astype(F32) + y[:, at] * factor * gains[1, k : k + 1, :]).astype(BF16)

    def run(step, *which):
        with jax.named_scope(step.__name__):
            step(*which)

    lead = qc // chunk
    with jax.named_scope("cachewait"):
        for b in range(ready, rows, part):
            settle(kbuf.at[pl.ds(b - ready, part)], ksem.at[b // part])
    for p in range(lead):
        run(split, p)
        for c in range(2):
            run(score, c, p)
    for c in range(lead, chunks):
        run(split, c)
    with jax.named_scope("valueswait"):
        for b in range(0, rows, part):
            settle(vbuf.at[pl.ds(b, part)], vsem.at[b // part])
    for c in range(CHUNKS):
        if 0 < c < CHUNKS - 1:
            for p in range(lead):
                run(score, c + 1, p)
        run(soft, c)
        run(mix, c)
    run(project, 0)
    for c in range(1, CHUNKS):
        run(project, c)
    for c in range(CHUNKS):
        run(total, c)
    for c in range(CHUNKS):
        run(finish, c)

    with jax.named_scope("drain"):
        settle(rbuf.at[pl.ds(1, n - 1)], s1)
        settle(pout, sp)
        settle(rs.at[pl.ds(1, half - 1)], s2)
        settle(gath.at[:, pl.ds(1, n - 1)], s3)

        for h in range(2):
            @pl.when(mt == middle[h])
            def _():
                settle(ps.at[:, 0], s4)
                for b in range(m):
                    count = half - 1 if (h, b) == (0, middle[0]) else half
                    settle(fr.at[:, pl.ds(0, count)], s5.at[b])

        @pl.when((mt < middle[0]) | (mt > middle[1]))
        def _():
            settle(ps, s4)


def store_kernel(hid_v, nk_v, nv_v, hid_out, nk_out, nv_out, sem):
    copies = [
        pltpu.make_async_copy(hid_v, hid_out, sem.at[0]),
        pltpu.make_async_copy(nk_v, nk_out, sem.at[1]),
        pltpu.make_async_copy(nv_v, nv_out, sem.at[2]),
    ]
    for move in copies:
        move.start()
    for move in copies:
        move.wait()


def per_device(
    n, m, tokens, lengths, positions, in_gain, q_weight, k_weight, v_weight, q_gain, k_gain,
    key_cache, value_cache, out_weight, post_gain,
):
    rows, width = tokens.shape
    depth, qc = q_weight.shape
    kc = k_weight.shape[1]
    cols = qc + 2 * kc
    chunks = cols // min(512, cols)
    heads = qc // HD
    ctx = key_cache.shape[1]
    ocols = out_weight.shape[1]
    part = rows // CHUNKS
    half = n // 2
    exponent = np.arange(HD // 2) * (2.0 / HD)
    frequency = np.power(rope_base, -exponent).astype(np.float32)
    frequency = np.concatenate([frequency, frequency])[None, :]

    full = pl.BlockSpec(memory_space=VMEM)
    anywhere = pl.BlockSpec(memory_space=pltpu.HBM)
    dma = pltpu.SemaphoreType.DMA
    results = [
        jax.ShapeDtypeStruct((rows, width), BF16),
        jax.ShapeDtypeStruct((rows, kc), BF16),
        jax.ShapeDtypeStruct((rows, kc), BF16),
    ]
    made = pl.pallas_call(
        functools.partial(layer_kernel, n, m),
        name="layer",
        out_shape=results,
        in_specs=[anywhere] * 14,
        out_specs=[full] * 3,
        scratch_shapes=[
            VMEM((rows, width), BF16),
            SMEM((rows,), jnp.int32),
            SMEM((rows,), jnp.int32),
            VMEM((3, 1, HD), F32),
            VMEM((2, width // HD, HD), F32),
            VMEM((depth, cols), BF16),
            VMEM((READY, ctx, kc), BF16),
            VMEM((rows, ctx, kc), BF16),
            VMEM((READY, kc, ctx), BF16),
            VMEM((ocols, qc), BF16),
            VMEM((qc, ocols), BF16),
            VMEM((n, rows, depth), BF16),
            VMEM((n, rows, depth), BF16),
            VMEM((half, rows, cols), F32),
            VMEM((half, rows, cols), BF16),
            VMEM((half, rows, cols), BF16),
            VMEM((half, rows, cols), BF16),
            VMEM((half, rows, cols), BF16),
            VMEM((rows, heads, HD), F32),
            VMEM((rows, kc // HD, HD), F32),
            VMEM((rows, kc // HD, HD), F32),
            VMEM((rows, heads, ctx), F32),
            VMEM((rows, heads, ctx), BF16),
            VMEM((rows, heads, HD), F32),
            VMEM((rows, heads, HD), F32),
            VMEM((rows, heads, HD), F32),
            VMEM((CHUNKS, part, qc), BF16),
            VMEM((CHUNKS, n, part, qc), BF16),
            VMEM((CHUNKS, 2, half * part, ocols), BF16),
            VMEM((CHUNKS, m, half * part, ocols), BF16),
            VMEM((CHUNKS, half, part, ocols), BF16),
            VMEM((CHUNKS, n, part, ocols), BF16),
            dma((5,)), dma((2,)), dma((CHUNKS,)), dma((CHUNKS,)), dma, dma, dma, dma, dma((chunks,)), dma, dma((chunks,)),
            dma, dma((CHUNKS,)), dma, dma((CHUNKS,)), dma((m,)), dma((CHUNKS,)),
        ],
        compiler_params=pltpu.CompilerParams(
            collective_id=0, has_side_effects=True, vmem_limit_bytes=LIMIT),
    )(*[pltpu.with_memory_space_constraint(operand, pltpu.HBM) for operand in (
        tokens, lengths, positions, jnp.asarray(frequency), in_gain.reshape(width // HD, HD),
        q_weight, k_weight, v_weight, q_gain[None, :], k_gain[None, :],
        key_cache, value_cache, out_weight.T, post_gain.reshape(width // HD, HD))])
    return pl.pallas_call(
        store_kernel,
        name="store",
        out_shape=results,
        in_specs=[full] * 3,
        out_specs=[anywhere] * 3,
        scratch_shapes=[dma((3,))],
        compiler_params=pltpu.CompilerParams(vmem_limit_bytes=1 << 20),
    )(*made)


def solution(mesh):
    n, m = mesh.shape["dp"], mesh.shape["tensor"]
    return jax.shard_map(
        functools.partial(per_device, n, m),
        mesh=mesh,
        in_specs=(
            P("dp", None),
            P("dp"),
            P("dp"),
            P(),
            P("dp", "tensor"),
            P("dp", "tensor"),
            P("dp", "tensor"),
            P(),
            P(),
            P("dp", None, "tensor"),
            P("dp", None, "tensor"),
            P("tensor", "dp"),
            P(),
        ),
        out_specs=(P("dp", None), P("dp", "tensor"), P("dp", "tensor")),
        check_vma=False,
    )
```
